32 devices in a mesh: row: 8 (over y, x, core), col: 4 (over z).
Axes of the slice: x: 2, y: 2, z: 4, core: 2. Of those that a mesh axis runs over, the one named last changes fastest.
Arguments:
- species: float32 [2, 256, 256, 128], P(None, None, 'row', 'col'), may hold values from -6 to 6
- coupling: float32 [2, 2], replicated, may hold values from -4 to 4
- symbol_x: float32 [256], replicated, may hold values from 0.3 to 3
- symbol_y: float32 [256], replicated, may hold values from 0.3 to 3
- symbol_z: float32 [128], replicated, may hold values from 0.3 to 3
Outputs:
- modes: float32 [2, 256, 256, 128], P(None, 'row', 'col')
The draws below stay inside these ranges and needn't reach their ends.
All inputs are finite; a program needn't handle non-finite values.
Results may differ from the reference program's by a relative error of at most 0.000078.
Values sent between devices are 32-bit elements.
A program may use at most 128 MiB of HBM per device.

```python
import jax
import jax.numpy as jnp
from jax import lax

GRID_X = 256
GRID_Y = 256
GRID_Z = 128
FIELDS = 2


def block_scale(own_key, shape, cuts, low, top_value):
    level, own = 1.0, jax.random.fold_in(own_key, 6)
    for position, shards_of in cuts:
        draws = jnp.exp(jax.random.uniform(jax.random.fold_in(own, position), (shards_of,), jnp.float32, low / len(cuts), top_value / len(cuts)))
        level = level * jnp.repeat(draws, shape[position] // shards_of).reshape([-1 if axis == position else 1 for axis in range(len(shape))])
    return level


def scatter_about(key, extent, width, limit, shards=(), kind=jnp.bfloat16):
    values = width * jax.random.normal(key, extent, jnp.float32)
    if shards:
        values = values * block_scale(key, extent, shards, -0.22, 0.18)
    return jnp.clip(values, -limit, limit).astype(kind)


def setup_inputs(seed: int = 0) -> dict:
    seeds = jax.random.split(jax.random.key(seed), 6)
    species = scatter_about(seeds[0], (FIELDS, GRID_X, GRID_Y, GRID_Z), 1.0, 6.0, ((2, 8), (3, 4)), jnp.float32)
    coupling = scatter_about(seeds[1], (FIELDS, FIELDS), 0.7, 4.0, (), jnp.float32)
    symbol_x = jnp.clip(jax.random.uniform(seeds[2], (GRID_X,), jnp.float32, 0.3, 3.0), 0.3, 3.0)
    symbol_y = jnp.clip(jax.random.uniform(seeds[3], (GRID_Y,), jnp.float32, 0.3, 3.0), 0.3, 3.0)
    symbol_z = jnp.clip(jax.random.uniform(seeds[4], (GRID_Z,), jnp.float32, 0.3, 3.0), 0.3, 3.0)
    return {"species": species, "coupling": coupling, "symbol_x": symbol_x, "symbol_y": symbol_y, "symbol_z": symbol_z}


def mode_table(count):
    rank = jnp.arange(count)
    angle = (jnp.pi / (count + 1)) * (((rank[:, None] + 1) * (rank[None, :] + 1)) % (2 * count + 2)).astype(jnp.float32)
    return jnp.sin(angle) * (2.0 / (count + 1)) ** 0.5


def transform_dim(values, dim):
    moved = jnp.tensordot(values, mode_table(values.shape[dim]), axes=([dim], [0]), precision=lax.Precision.HIGHEST)
    return jnp.moveaxis(moved, -1, dim)


def reference(species, coupling, symbol_x, symbol_y, symbol_z):
    modes = species
    modes = transform_dim(modes, 1)
    modes = transform_dim(modes, 2)
    modes = transform_dim(modes, 3)
    symbol = symbol_x[:, None, None] + symbol_y[None, :, None] + symbol_z[None, None, :]
    weight_xyz = 1.0 / (1.0 + symbol)
    mixed_fields = jnp.einsum("ab,bxyz->axyz", coupling, modes, precision=lax.Precision.HIGHEST)
    modes = weight_xyz * modes + (1.0 - weight_xyz) * mixed_fields
    return modes
```

```python
import functools

import jax
import jax.numpy as jnp
import numpy as np
from jax import lax
from jax.experimental import pallas as pl
from jax.experimental.pallas import tpu as pltpu
from jax.sharding import PartitionSpec as P

MESH = pl.DeviceIdType.MESH
LANES = 128
SUB = 8


def mode_table(count):
    rank = np.arange(1, count + 1)
    angle = np.pi / (count + 1) * ((rank[:, None] * rank[None, :]) % (2 * count + 2))
    return (np.sin(angle) * np.sqrt(2.0 / (count + 1))).astype(np.float32)


def halves_of(table):
    high = table.astype(jnp.bfloat16)
    low = (table - high.astype(np.float32)).astype(jnp.bfloat16)
    return high, low


def halves(values):
    high = values.astype(jnp.bfloat16)
    low = (values - high.astype(jnp.float32)).astype(jnp.bfloat16)
    return high, low


def partner(me, step, count):
    if count & (count - 1):
        return lax.rem(me + step, count)
    other, bit = me, 1
    while bit < count:
        if step & bit:
            other = other + bit * (1 - 2 * lax.rem(me // bit, 2))
        bit *= 2
    return other


def swap_groups(parts):
    parts = list(parts)
    count = len(parts)
    width = LANES // count
    lane = lax.broadcasted_iota(jnp.int32, parts[0].shape, 1)
    step = count // 2
    while step:
        keep = lax.rem(lane // (width * step), 2) == 0
        for first in range(count):
            if first & step:
                continue
            a, b = parts[first], parts[first + step]
            parts[first] = jnp.where(keep, a, pltpu.roll(b, width * step, 1))
            parts[first + step] = jnp.where(keep, pltpu.roll(a, LANES - width * step, 1), b)
        step //= 2
    return parts


def kernel(sizes, a_ref, hx_ref, hy_ref, hz_ref, o_ref, t_ref, r_ref, v_ref, w_ref,
           send_row, recv_row, send_col, recv_col, own_row, own_col):
    rows, cols, fields, nx, ny, nz = sizes
    share_y = ny // cols
    groups = LANES // (nz // cols)
    blocks = ny // rows // groups
    chunks = nx // rows // SUB
    quads = SUB // groups
    total = fields * chunks
    slab = blocks * SUB
    row, col = lax.axis_index("row"), lax.axis_index("col")

    barrier = pltpu.get_barrier_semaphore()
    for step in range(1, rows):
        pl.semaphore_signal(barrier, inc=1, device_id={"row": partner(row, step, rows)}, device_id_type=MESH)
    for step in range(1, cols):
        pl.semaphore_signal(barrier, inc=1, device_id={"col": partner(col, step, cols)}, device_id_type=MESH)

    def row_copy(i, step):
        to = partner(row, step, rows)
        return pltpu.make_async_remote_copy(
            src_ref=t_ref.at[i, to], dst_ref=r_ref.at[i, pl.ds(row * slab, slab)],
            send_sem=send_row.at[i, step], recv_sem=recv_row.at[i, step],
            device_id={"row": to}, device_id_type=MESH)

    def own_row_copy(i):
        return pltpu.make_async_copy(
            t_ref.at[i, row], r_ref.at[i, pl.ds(row * slab, slab)], own_row.at[i])

    def col_copy(i, step):
        to = partner(col, step, cols)
        return pltpu.make_async_remote_copy(
            src_ref=v_ref.at[i, to], dst_ref=w_ref.at[i, col],
            send_sem=send_col.at[i, step], recv_sem=recv_col.at[i, step],
            device_id={"col": to}, device_id_type=MESH)

    def own_col_copy(i):
        return pltpu.make_async_copy(v_ref.at[i, col], w_ref.at[i, col], own_col.at[i])

    per_dot = 2
    for f in range(fields):
        for n in range(blocks // per_dot):
            width = per_dot * LANES
            high, low = halves(a_ref[f, n * width:(n + 1) * width, :])
            part = lax.dot_general(
                hx_ref[...], jnp.concatenate([high, high, low], axis=1),
                (((1,), (1,)), ((), ())), preferred_element_type=jnp.float32)
            part = part.reshape(rows, chunks, SUB, width)
            for j in range(chunks):
                for b in range(per_dot):
                    at = (n * per_dot + b) * SUB
                    t_ref[f * chunks + j, :, at:at + SUB, :] = part[:, j, :, b * LANES:(b + 1) * LANES]
        if f == 0:
            pl.semaphore_wait(barrier, rows + cols - 2)
        for j in range(chunks):
            for step in range(rows - 1, 0, -1):
                row_copy(f * chunks + j, step).start()
            own_row_copy(f * chunks + j).start()

    def y_step(i, carry):
        for step in range(rows - 1, 0, -1):
            row_copy(i, step).wait_recv()
        own_row_copy(i).wait()
        whole = []
        for q in range(quads):
            parts = [r_ref[i, pl.ds(q * groups + g, rows * blocks, stride=SUB), :] for g in range(groups)]
            whole.append(jnp.concatenate(swap_groups(parts), axis=0))
        high, low = halves(jnp.concatenate(whole, axis=1))
        got = jnp.dot(hy_ref[...], jnp.concatenate([high, high, low], axis=0),
                      preferred_element_type=jnp.float32)
        for c in range(cols):
            for q in range(quads):
                v_ref[i, c, q * share_y:(q + 1) * share_y, :] = got[
                    c * share_y:(c + 1) * share_y, q * LANES:(q + 1) * LANES]
        for step in range(cols - 1, 0, -1):
            col_copy(i, step).start()
        own_col_copy(i).start()
        return carry

    lax.fori_loop(0, total, y_step, 0)

    def z_step(i, carry):
        for step in range(cols - 1, 0, -1):
            col_copy(i, step).wait_recv()
        own_col_copy(i).wait()
        lines = []
        for q in range(quads):
            tiles = []
            for c in range(0, cols, groups):
                tiles.append(swap_groups(
                    [w_ref[i, c + g, q * share_y:(q + 1) * share_y, :] for g in range(groups)]))
            for k in range(groups):
                lines.append(jnp.concatenate([tile[k] for tile in tiles], axis=1))
        high, low = halves(jnp.concatenate(lines, axis=0))
        got = jnp.dot(jnp.concatenate([high, low], axis=1), hz_ref[...],
                      preferred_element_type=jnp.float32)
        got = (got[:, :nz] + got[:, nz:]).reshape(SUB, share_y, nz)
        o_ref[i // chunks, pl.ds(lax.rem(i, chunks) * SUB, SUB)] = got
        return carry

    lax.fori_loop(0, total, z_step, 0)

    def drain(i, carry):
        for step in range(1, rows):
            row_copy(i, step).wait_send()
        for step in range(1, cols):
            col_copy(i, step).wait_send()
        return carry

    lax.fori_loop(0, total, drain, 0)


def local(rows, cols, species, coupling, symbol_x, symbol_y, symbol_z):
    fields, nx, near_y, near_z = species.shape
    ny, nz = near_y * rows, near_z * cols
    share_x, share_y = nx // rows, ny // cols
    groups = LANES // near_z
    blocks = near_y // groups
    total = fields * share_x // SUB

    high, low = halves_of(mode_table(nx))
    hx = np.concatenate([high, low, high], axis=1)
    order = np.arange(ny).reshape(rows, blocks, groups).transpose(2, 0, 1).reshape(-1)
    high, low = halves_of(mode_table(ny)[:, order])
    hy = np.concatenate([high, low, high], axis=1)
    high, low = halves_of(mode_table(nz))
    hz = np.concatenate([np.concatenate([high, low], axis=1),
                         np.concatenate([high, np.zeros_like(low)], axis=1)], axis=0)

    lines = jnp.transpose(species, (0, 2, 3, 1)).reshape(fields, near_y * near_z, nx)
    vmem = pl.BlockSpec(memory_space=pltpu.VMEM)
    dma = pltpu.SemaphoreType.DMA
    modes = pl.pallas_call(
        functools.partial(kernel, (rows, cols, fields, nx, ny, nz)),
        out_shape=jax.ShapeDtypeStruct((fields, share_x, share_y, nz), jnp.float32),
        in_specs=[vmem] * 4,
        out_specs=vmem,
        scratch_shapes=[
            pltpu.VMEM((total, rows, blocks * SUB, LANES), jnp.float32),
            pltpu.VMEM((total, rows * blocks * SUB, LANES), jnp.float32),
            pltpu.VMEM((total, cols, SUB // groups * share_y, LANES), jnp.float32),
            pltpu.VMEM((total, cols, SUB // groups * share_y, LANES), jnp.float32),
            dma((total, rows)), dma((total, rows)),
            dma((total, cols)), dma((total, cols)),
            dma((total,)), dma((total,)),
        ],
        compiler_params=pltpu.CompilerParams(
            collective_id=0, has_side_effects=True, vmem_limit_bytes=56 * 2**20),
    )(lines, jnp.asarray(hx), jnp.asarray(hy), jnp.asarray(hz))

    part_x = lax.dynamic_slice_in_dim(symbol_x, lax.axis_index("row") * share_x, share_x)
    part_y = lax.dynamic_slice_in_dim(symbol_y, lax.axis_index("col") * share_y, share_y)
    symbol = part_x[:, None, None] + part_y[None, :, None] + symbol_z[None, None, :]
    weight = 1.0 / (1.0 + symbol)
    mixed = sum(coupling[:, b, None, None, None] * modes[b][None] for b in range(fields))
    return weight * modes + (1.0 - weight) * mixed


def solution(mesh):
    return jax.shard_map(
        functools.partial(local, mesh.shape["row"], mesh.shape["col"]),
        mesh=mesh,
        in_specs=(P(None, None, "row", "col"), P(), P(), P(), P()),
        out_specs=P(None, "row", "col", None),
        check_vma=False,
    )
```

```python
import functools

import jax
import jax.numpy as jnp
import numpy as np
from jax import lax
from jax.experimental import pallas as pl
from jax.experimental.pallas import tpu as pltpu
from jax.sharding import PartitionSpec as P

MESH = pl.DeviceIdType.MESH
LANES = 128
SUB = 8


def mode_table(count):
    rank = np.arange(1, count + 1)
    angle = np.pi / (count + 1) * ((rank[:, None] * rank[None, :]) % (2 * count + 2))
    return (np.sin(angle) * np.sqrt(2.0 / (count + 1))).astype(np.float32)


def halves_of(table):
    high = table.astype(jnp.bfloat16)
    low = (table - high.astype(np.float32)).astype(jnp.bfloat16)
    return high, low


def halves(values):
    high = values.astype(jnp.bfloat16)
    low = (values - high.astype(jnp.float32)).astype(jnp.bfloat16)
    return high, low


def partner(me, step, count):
    if count & (count - 1):
        return lax.rem(me + step, count)
    other, bit = me, 1
    while bit < count:
        if step & bit:
            other = other + bit * (1 - 2 * lax.rem(me // bit, 2))
        bit *= 2
    return other


def swap_groups(parts):
    parts = list(parts)
    count = len(parts)
    width = LANES // count
    lane = lax.broadcasted_iota(jnp.int32, parts[0].shape, 1)
    step = count // 2
    while step:
        keep = lax.rem(lane // (width * step), 2) == 0
        for first in range(count):
            if first & step:
                continue
            a, b = parts[first], parts[first + step]
            parts[first] = jnp.where(keep, a, pltpu.roll(b, width * step, 1))
            parts[first + step] = jnp.where(keep, pltpu.roll(a, LANES - width * step, 1), b)
        step //= 2
    return parts


def kernel(sizes, coupling_ref, sx_ref, a_hbm, hx_hbm, hy_hbm, hz_hbm, sy_ref, sz_ref, o_hbm,
           a_ref, hx_ref, hy_ref, hz_ref, sy_rows, m_ref, o_ref, t_ref, r_ref, v_ref, w_ref,
           load_a, load_h, store_o, send_row, recv_row, send_col, recv_col, own_row, own_col):
    rows, cols, fields, nx, ny, nz = sizes
    share_y = ny // cols
    groups = LANES // (nz // cols)
    blocks = ny // rows // groups
    chunks = nx // rows // SUB
    quads = SUB // groups
    total = fields * chunks
    slab = blocks * SUB
    row, col = lax.axis_index("row"), lax.axis_index("col")
    per_dot = 2
    width = per_dot * LANES
    pieces = blocks // per_dot

    def load(f, n):
        at = pl.ds(n * width, width)
        return pltpu.make_async_copy(a_hbm.at[f, at], a_ref.at[f, at], load_a.at[f, n])

    tables = [pltpu.make_async_copy(src, dst, load_h.at[n]) for n, (src, dst) in enumerate(
        ((hx_hbm, hx_ref), (hy_hbm, hy_ref), (hz_hbm, hz_ref)))]
    tables[0].start()
    for f in range(fields):
        for n in range(pieces):
            load(f, n).start()
    tables[1].start()
    tables[2].start()

    barrier = pltpu.get_barrier_semaphore()
    for step in range(1, rows):
        pl.semaphore_signal(barrier, inc=1, device_id={"row": partner(row, step, rows)}, device_id_type=MESH)
    for step in range(1, cols):
        pl.semaphore_signal(barrier, inc=1, device_id={"col": partner(col, step, cols)}, device_id_type=MESH)

    def row_copy(i, step):
        to = partner(row, step, rows)
        return pltpu.make_async_remote_copy(
            src_ref=t_ref.at[i, to], dst_ref=r_ref.at[i, pl.ds(row * slab, slab)],
            send_sem=send_row.at[i, step], recv_sem=recv_row.at[i, step],
            device_id={"row": to}, device_id_type=MESH)

    def own_row_copy(i):
        return pltpu.make_async_copy(
            t_ref.at[i, row], r_ref.at[i, pl.ds(row * slab, slab)], own_row.at[i])

    def col_copy(i, step):
        to = partner(col, step, cols)
        return pltpu.make_async_remote_copy(
            src_ref=v_ref.at[i, to], dst_ref=w_ref.at[i, col],
            send_sem=send_col.at[i, step], recv_sem=recv_col.at[i, step],
            device_id={"col": to}, device_id_type=MESH)

    def own_col_copy(i):
        return pltpu.make_async_copy(v_ref.at[i, col], w_ref.at[i, col], own_col.at[i])

    tables[0].wait()
    for f in range(fields):
        for n in range(pieces):
            load(f, n).wait()
            high, low = halves(a_ref[f, n * width:(n + 1) * width, :])
            part = lax.dot_general(
                hx_ref[...], jnp.concatenate([high, high, low], axis=1),
                (((1,), (1,)), ((), ())), preferred_element_type=jnp.float32)
            part = part.reshape(rows, chunks, SUB, width)
            for j in range(chunks):
                for b in range(per_dot):
                    at = (n * per_dot + b) * SUB
                    t_ref[f * chunks + j, :, at:at + SUB, :] = part[:, j, :, b * LANES:(b + 1) * LANES]
        if f == 0:
            pl.semaphore_wait(barrier, rows + cols - 2)
        for j in range(chunks):
            for step in range(rows - 1, 0, -1):
                row_copy(f * chunks + j, step).start()
            own_row_copy(f * chunks + j).start()

    tables[1].wait()

    def y_step(i, carry):
        for step in range(rows - 1, 0, -1):
            row_copy(i, step).wait_recv()
        own_row_copy(i).wait()
        whole = []
        for q in range(quads):
            parts = [r_ref[i, pl.ds(q * groups + g, rows * blocks, stride=SUB), :] for g in range(groups)]
            whole.append(jnp.concatenate(swap_groups(parts), axis=0))
        high, low = halves(jnp.concatenate(whole, axis=1))
        got = jnp.dot(hy_ref[...], jnp.concatenate([high, high, low], axis=0),
                      preferred_element_type=jnp.float32)
        for c in range(cols):
            for q in range(quads):
                v_ref[i, c, q * share_y:(q + 1) * share_y, :] = got[
                    c * share_y:(c + 1) * share_y, q * LANES:(q + 1) * LANES]
        for step in range(cols - 1, 0, -1):
            col_copy(i, step).start()
        own_col_copy(i).start()
        return carry

    lax.fori_loop(0, total, y_step, 0)

    tables[2].wait()
    for n in range(ny // LANES):
        at = slice(n * LANES, (n + 1) * LANES)
        sy_rows[at, :] = jnp.broadcast_to(sy_ref[:, at], (LANES, LANES)).T

    def modes_of(i):
        for step in range(cols - 1, 0, -1):
            col_copy(i, step).wait_recv()
        own_col_copy(i).wait()
        lines = []
        for q in range(quads):
            tiles = []
            for c in range(0, cols, groups):
                tiles.append(swap_groups(
                    [w_ref[i, c + g, q * share_y:(q + 1) * share_y, :] for g in range(groups)]))
            for k in range(groups):
                lines.append(jnp.concatenate([tile[k] for tile in tiles], axis=1))
        high, low = halves(jnp.concatenate(lines, axis=0))
        got = jnp.dot(jnp.concatenate([high, low], axis=1), hz_ref[...],
                      preferred_element_type=jnp.float32)
        return got[:, :nz] + got[:, nz:]

    def z_step(i, carry):
        m_ref[i] = modes_of(i)
        return carry

    lax.fori_loop(0, total - chunks, z_step, 0)

    def store(j):
        at = pl.ds(j * SUB, SUB)
        return pltpu.make_async_copy(o_ref.at[:, at], o_hbm.at[:, at], store_o.at[j])

    def last_step(j, carry):
        last = modes_of(total - chunks + j)
        lines_y = sy_rows[pl.ds(col * share_y, share_y), :]
        lines_y = jnp.concatenate([lines_y] * (nz // LANES), axis=1) + sz_ref[...]
        for k in range(SUB):
            at = slice(k * share_y, (k + 1) * share_y)
            weight = 1.0 / (1.0 + (sx_ref[row * (chunks * SUB) + j * SUB + k] + lines_y))
            old = [m_ref[f * chunks + j, at, :] for f in range(fields - 1)] + [last[at, :]]
            for f in range(fields):
                mixed = coupling_ref[f, 0] * old[0]
                for b in range(1, fields):
                    mixed = mixed + coupling_ref[f, b] * old[b]
                o_ref[f, j * SUB + k] = weight * old[f] + (1.0 - weight) * mixed
        store(j).start()
        return carry

    lax.fori_loop(0, chunks, last_step, 0)

    def drain(i, carry):
        for step in range(1, rows):
            row_copy(i, step).wait_send()
        for step in range(1, cols):
            col_copy(i, step).wait_send()
        return carry

    lax.fori_loop(0, total, drain, 0)
    for j in range(chunks):
        store(j).wait()


def local(rows, cols, species, coupling, symbol_x, symbol_y, symbol_z):
    fields, nx, near_y, near_z = species.shape
    ny, nz = near_y * rows, near_z * cols
    share_x, share_y = nx // rows, ny // cols
    groups = LANES // near_z
    blocks = near_y // groups
    total = fields * share_x // SUB

    high, low = halves_of(mode_table(nx))
    hx = np.concatenate([high, low, high], axis=1)
    order = np.arange(ny).reshape(rows, blocks, groups).transpose(2, 0, 1).reshape(-1)
    high, low = halves_of(mode_table(ny)[:, order])
    hy = np.concatenate([high, low, high], axis=1)
    high, low = halves_of(mode_table(nz))
    hz = np.concatenate([np.concatenate([high, low], axis=1),
                         np.concatenate([high, np.zeros_like(low)], axis=1)], axis=0)

    lines = jnp.transpose(species, (0, 2, 3, 1)).reshape(fields, near_y * near_z, nx)
    vmem = pl.BlockSpec(memory_space=pltpu.VMEM)
    smem = pl.BlockSpec(memory_space=pltpu.SMEM)
    hbm = pl.BlockSpec(memory_space=pltpu.HBM)
    dma = pltpu.SemaphoreType.DMA
    f32 = jnp.float32
    chunks = total // fields
    return pl.pallas_call(
        functools.partial(kernel, (rows, cols, fields, nx, ny, nz)),
        out_shape=jax.ShapeDtypeStruct((fields, share_x, share_y, nz), f32),
        in_specs=[smem, smem, hbm, hbm, hbm, hbm, vmem, vmem],
        out_specs=hbm,
        scratch_shapes=[
            pltpu.VMEM(lines.shape, f32),
            pltpu.VMEM(hx.shape, hx.dtype),
            pltpu.VMEM(hy.shape, hy.dtype),
            pltpu.VMEM(hz.shape, hz.dtype),
            pltpu.VMEM((ny, LANES), f32),
            pltpu.VMEM((max(total - chunks, 1), SUB * share_y, nz), f32),
            pltpu.VMEM((fields, share_x, share_y, nz), f32),
            pltpu.VMEM((total, rows, blocks * SUB, LANES), f32),
            pltpu.VMEM((total, rows * blocks * SUB, LANES), f32),
            pltpu.VMEM((total, cols, SUB // groups * share_y, LANES), f32),
            pltpu.VMEM((total, cols, SUB // groups * share_y, LANES), f32),
            dma((fields, blocks // 2)), dma((3,)), dma((chunks,)),
            dma((total, rows)), dma((total, rows)),
            dma((total, cols)), dma((total, cols)),
            dma((total,)), dma((total,)),
        ],
        compiler_params=pltpu.CompilerParams(
            collective_id=0, has_side_effects=True, vmem_limit_bytes=60 * 2**20),
    )(coupling, symbol_x, lines, jnp.asarray(hx), jnp.asarray(hy), jnp.asarray(hz),
      symbol_y[None, :], symbol_z[None, :])


def solution(mesh):
    return jax.shard_map(
        functools.partial(local, mesh.shape["row"], mesh.shape["col"]),
        mesh=mesh,
        in_specs=(P(None, None, "row", "col"), P(), P(), P(), P()),
        out_specs=P(None, "row", "col", None),
        check_vma=False,
    )
```

```python
import functools

import jax
import jax.numpy as jnp
import numpy as np
from jax import lax
from jax.experimental import pallas as pl
from jax.experimental.pallas import tpu as pltpu
from jax.sharding import PartitionSpec as P

MESH = pl.DeviceIdType.MESH
LANES = 128
SUB = 8


def mode_table(count):
    rank = np.arange(1, count + 1)
    angle = np.pi / (count + 1) * ((rank[:, None] * rank[None, :]) % (2 * count + 2))
    return (np.sin(angle) * np.sqrt(2.0 / (count + 1))).astype(np.float32)


def halves_of(table):
    high = table.astype(jnp.bfloat16)
    low = (table - high.astype(np.float32)).astype(jnp.bfloat16)
    return high, low


def halves(values):
    high = values.astype(jnp.bfloat16)
    low = (values - high.astype(jnp.float32)).astype(jnp.bfloat16)
    return high, low


def partner(me, step, count):
    if count & (count - 1):
        return lax.rem(me + step, count)
    other, bit = me, 1
    while bit < count:
        if step & bit:
            other = other + bit * (1 - 2 * lax.rem(me // bit, 2))
        bit *= 2
    return other


def swap_groups(parts):
    parts = list(parts)
    count = len(parts)
    width = LANES // count
    lane = lax.broadcasted_iota(jnp.int32, parts[0].shape, 1)
    step = count // 2
    while step:
        keep = lax.rem(lane // (width * step), 2) == 0
        for first in range(count):
            if first & step:
                continue
            a, b = parts[first], parts[first + step]
            parts[first] = jnp.where(keep, a, pltpu.roll(b, width * step, 1))
            parts[first + step] = jnp.where(keep, pltpu.roll(a, LANES - width * step, 1), b)
        step //= 2
    return parts


def kernel(sizes, coupling_ref, sx_ref, a_hbm, hx_hbm, hy_hbm, hz_hbm, sy_ref, sz_ref, o_ref,
           a_ref, hx_ref, hy_ref, hz_ref, sy_rows, m_ref, t_ref, r_ref, v_ref, w_ref,
           load_a, load_h, send_row, recv_row, send_col, recv_col, own_row, own_col):
    rows, cols, fields, nx, ny, nz = sizes
    share_y = ny // cols
    groups = LANES // (nz // cols)
    blocks = ny // rows // groups
    chunks = nx // rows // SUB
    quads = SUB // groups
    total = fields * chunks
    slab = blocks * SUB
    row, col = lax.axis_index("row"), lax.axis_index("col")
    per_dot = 2
    width = per_dot * LANES
    pieces = blocks // per_dot

    def load(f, n):
        at = pl.ds(n * width, width)
        return pltpu.make_async_copy(a_hbm.at[f, at], a_ref.at[f, at], load_a.at[f, n])

    tables = [pltpu.make_async_copy(src, dst, load_h.at[n]) for n, (src, dst) in enumerate(
        ((hx_hbm, hx_ref), (hy_hbm, hy_ref), (hz_hbm, hz_ref)))]
    tables[0].start()
    for f in range(fields):
        for n in range(pieces):
            load(f, n).start()
    tables[1].start()
    tables[2].start()

    barrier = pltpu.get_barrier_semaphore()
    for step in range(1, rows):
        pl.semaphore_signal(barrier, inc=1, device_id={"row": partner(row, step, rows)}, device_id_type=MESH)
    for step in range(1, cols):
        pl.semaphore_signal(barrier, inc=1, device_id={"col": partner(col, step, cols)}, device_id_type=MESH)

    def row_copy(i, step):
        to = partner(row, step, rows)
        return pltpu.make_async_remote_copy(
            src_ref=t_ref.at[i, to], dst_ref=r_ref.at[i, pl.ds(row * slab, slab)],
            send_sem=send_row.at[i, step], recv_sem=recv_row.at[i, step],
            device_id={"row": to}, device_id_type=MESH)

    def own_row_copy(i):
        return pltpu.make_async_copy(
            t_ref.at[i, row], r_ref.at[i, pl.ds(row * slab, slab)], own_row.at[i])

    def col_copy(i, step):
        to = partner(col, step, cols)
        return pltpu.make_async_remote_copy(
            src_ref=v_ref.at[i, to], dst_ref=w_ref.at[i, col],
            send_sem=send_col.at[i, step], recv_sem=recv_col.at[i, step],
            device_id={"col": to}, device_id_type=MESH)

    def own_col_copy(i):
        return pltpu.make_async_copy(v_ref.at[i, col], w_ref.at[i, col], own_col.at[i])

    tables[0].wait()
    span = rows * SUB
    arrived = set()
    for f in range(fields):
        for low_j, top_j in ((0, 1), (1, chunks)) if f == 0 else ((0, chunks),):
            for n in range(pieces):
                if (f, n) not in arrived:
                    load(f, n).wait()
                    arrived.add((f, n))
                high, low = halves(a_ref[f, n * width:(n + 1) * width, :])
                part = lax.dot_general(
                    hx_ref[low_j * span:top_j * span, :], jnp.concatenate([high, high, low], axis=1),
                    (((1,), (1,)), ((), ())), preferred_element_type=jnp.float32)
                part = part.reshape(top_j - low_j, rows, SUB, width)
                for j in range(low_j, top_j):
                    for b in range(per_dot):
                        at = (n * per_dot + b) * SUB
                        t_ref[f * chunks + j, :, at:at + SUB, :] = part[
                            j - low_j, :, :, b * LANES:(b + 1) * LANES]
            if not f and not low_j:
                pl.semaphore_wait(barrier, rows + cols - 2)
            for j in range(low_j, top_j):
                for step in range(rows - 1, 0, -1):
                    row_copy(f * chunks + j, step).start()
                own_row_copy(f * chunks + j).start()

    tables[1].wait()

    def y_step(i, carry):
        for step in range(rows - 1, 0, -1):
            row_copy(i, step).wait_recv()
        own_row_copy(i).wait()
        whole = []
        for q in range(quads):
            parts = [r_ref[i, pl.ds(q * groups + g, rows * blocks, stride=SUB), :] for g in range(groups)]
            whole.append(jnp.concatenate(swap_groups(parts), axis=0))
        high, low = halves(jnp.concatenate(whole, axis=1))
        got = jnp.dot(hy_ref[...], jnp.concatenate([high, high, low], axis=0),
                      preferred_element_type=jnp.float32)
        for c in range(cols):
            for q in range(quads):
                v_ref[i, c, q * share_y:(q + 1) * share_y, :] = got[
                    c * share_y:(c + 1) * share_y, q * LANES:(q + 1) * LANES]
        for step in range(cols - 1, 0, -1):
            col_copy(i, step).start()
        own_col_copy(i).start()
        return carry

    lax.fori_loop(0, total, y_step, 0)

    tables[2].wait()
    for n in range(ny // LANES):
        at = slice(n * LANES, (n + 1) * LANES)
        sy_rows[at, :] = jnp.broadcast_to(sy_ref[:, at], (LANES, LANES)).T

    def modes_of(i):
        for step in range(cols - 1, 0, -1):
            col_copy(i, step).wait_recv()
        own_col_copy(i).wait()
        lines = []
        for q in range(quads):
            tiles = []
            for c in range(0, cols, groups):
                tiles.append(swap_groups(
                    [w_ref[i, c + g, q * share_y:(q + 1) * share_y, :] for g in range(groups)]))
            for k in range(groups):
                lines.append(jnp.concatenate([tile[k] for tile in tiles], axis=1))
        high, low = halves(jnp.concatenate(lines, axis=0))
        got = jnp.dot(jnp.concatenate([high, low], axis=1), hz_ref[...],
                      preferred_element_type=jnp.float32)
        return got[:, :nz] + got[:, nz:]

    def z_step(i, carry):
        m_ref[i] = modes_of(i)
        return carry

    lax.fori_loop(0, total - chunks, z_step, 0)

    def last_step(j, carry):
        last = modes_of(total - chunks + j)
        lines_y = sy_rows[pl.ds(col * share_y, share_y), :]
        lines_y = jnp.concatenate([lines_y] * (nz // LANES), axis=1) + sz_ref[...]
        for k in range(SUB):
            at = slice(k * share_y, (k + 1) * share_y)
            weight = 1.0 / (1.0 + (sx_ref[row * (chunks * SUB) + j * SUB + k] + lines_y))
            old = [m_ref[f * chunks + j, at, :] for f in range(fields - 1)] + [last[at, :]]
            for f in range(fields):
                mixed = coupling_ref[f, 0] * old[0]
                for b in range(1, fields):
                    mixed = mixed + coupling_ref[f, b] * old[b]
                o_ref[f, j * SUB + k] = weight * old[f] + (1.0 - weight) * mixed
        return carry

    lax.fori_loop(0, chunks, last_step, 0)

    def drain(i, carry):
        for step in range(1, rows):
            row_copy(i, step).wait_send()
        for step in range(1, cols):
            col_copy(i, step).wait_send()
        return carry

    lax.fori_loop(0, total, drain, 0)


def local(rows, cols, species, coupling, symbol_x, symbol_y, symbol_z):
    fields, nx, near_y, near_z = species.shape
    ny, nz = near_y * rows, near_z * cols
    share_x, share_y = nx // rows, ny // cols
    groups = LANES // near_z
    blocks = near_y // groups
    total = fields * share_x // SUB

    order = np.arange(nx).reshape(rows, share_x // SUB, SUB).transpose(1, 0, 2).reshape(-1)
    high, low = halves_of(mode_table(nx)[order])
    hx = np.concatenate([high, low, high], axis=1)
    order = np.arange(ny).reshape(rows, blocks, groups).transpose(2, 0, 1).reshape(-1)
    high, low = halves_of(mode_table(ny)[:, order])
    hy = np.concatenate([high, low, high], axis=1)
    high, low = halves_of(mode_table(nz))
    hz = np.concatenate([np.concatenate([high, low], axis=1),
                         np.concatenate([high, np.zeros_like(low)], axis=1)], axis=0)

    lines = jnp.transpose(species, (0, 2, 3, 1)).reshape(fields, near_y * near_z, nx)
    vmem = pl.BlockSpec(memory_space=pltpu.VMEM)
    smem = pl.BlockSpec(memory_space=pltpu.SMEM)
    hbm = pl.BlockSpec(memory_space=pltpu.HBM)
    dma = pltpu.SemaphoreType.DMA
    f32 = jnp.float32
    chunks = total // fields
    return pl.pallas_call(
        functools.partial(kernel, (rows, cols, fields, nx, ny, nz)),
        out_shape=pltpu.VMEM((fields, share_x, share_y, nz), f32),
        in_specs=[smem, smem, hbm, hbm, hbm, hbm, vmem, vmem],
        out_specs=vmem,
        scratch_shapes=[
            pltpu.VMEM(lines.shape, f32),
            pltpu.VMEM(hx.shape, hx.dtype),
            pltpu.VMEM(hy.shape, hy.dtype),
            pltpu.VMEM(hz.shape, hz.dtype),
            pltpu.VMEM((ny, LANES), f32),
            pltpu.VMEM((max(total - chunks, 1), SUB * share_y, nz), f32),
            pltpu.VMEM((total, rows, blocks * SUB, LANES), f32),
            pltpu.VMEM((total, rows * blocks * SUB, LANES), f32),
            pltpu.VMEM((total, cols, SUB // groups * share_y, LANES), f32),
            pltpu.VMEM((total, cols, SUB // groups * share_y, LANES), f32),
            dma((fields, blocks // 2)), dma((3,)),
            dma((total, rows)), dma((total, rows)),
            dma((total, cols)), dma((total, cols)),
            dma((total,)), dma((total,)),
        ],
        compiler_params=pltpu.CompilerParams(
            collective_id=0, has_side_effects=True, vmem_limit_bytes=56 * 2**20),
    )(coupling, symbol_x, lines, jnp.asarray(hx), jnp.asarray(hy), jnp.asarray(hz),
      symbol_y[None, :], symbol_z[None, :])


def solution(mesh):
    return jax.shard_map(
        functools.partial(local, mesh.shape["row"], mesh.shape["col"]),
        mesh=mesh,
        in_specs=(P(None, None, "row", "col"), P(), P(), P(), P()),
        out_specs=P(None, "row", "col", None),
        check_vma=False,
    )
```
